32 devices in a mesh: dp: 8 (over y, x, core), tensor: 4 (over z).
Axes of the slice: x: 2, y: 2, z: 4, core: 2. Of those that a mesh axis runs over, the one named last changes fastest.
Arguments:
- hidden_states: bfloat16 [3072, 1536], P('dp', 'tensor'), may hold values from -1000 to 1000
- norm_gain: bfloat16 [1536], P('tensor'), may hold values from 0.5 to 1.5
- embedding: bfloat16 [19456, 1536], P(('dp', 'tensor')), may hold values from -2 to 2
- labels: int32 [3072], P('dp'), may hold values from 0 to 19455, as said below
Outputs:
- scores: float32 [3072], P('dp')
The draws below stay inside these ranges and needn't reach their ends.
Inputs may be any that keep to these rules, and one draw needn't show every extreme that they name: `labels`: A label may be any vocabulary entry.
All inputs are finite; a program needn't handle non-finite values.
Results may differ from the reference program's by a relative error of at most 0.0012.
Values may be sent and summed in bfloat16 or wider, within the bound.
No kernel may reach another device: no remote copies, remote signals or barrier semaphores. Data moves between devices by JAX's collectives and lax.ppermute only.
A program may use at most 64 MiB of HBM per device.

```python
import math
import jax
import jax.numpy as jnp
from jax import lax

D = 1536
VOCAB = 19456
TOKENS = 3072


def drawn_ids(key):
    vocab_step = VOCAB // 16
    token_step = TOKENS // 8
    ranks = jnp.arange(8, dtype=jnp.int32)
    picks = 2 * (ranks * vocab_step + jax.random.randint(jax.random.fold_in(key, 12), (8,), 0, vocab_step))
    positions = ranks * token_step + jax.random.randint(jax.random.fold_in(key, 25), (8,), 0, token_step)
    return (picks, positions)


def label_ids(key):
    base = jax.random.randint(jax.random.fold_in(key, 31), (TOKENS,), 0, VOCAB)
    picks, positions = drawn_ids(key)
    parity = jnp.arange(8, dtype=jnp.int32) % 2
    return base.at[positions].set(picks + parity)


def aligned_share(key):
    chosen_rows = jax.random.randint(jax.random.fold_in(key, 32), (TOKENS,), 0, 4) == 0
    target = jax.random.uniform(jax.random.fold_in(key, 33), (TOKENS,), jnp.float32, 10.0, 45.0)
    strength = target / (4.2 * math.sqrt(D))
    return jnp.where(chosen_rows, strength, 0.0)[:, None]


def embed_table(key):
    spread_scale = 5.0 / math.sqrt(D)
    table = jnp.clip(jax.random.normal(jax.random.fold_in(key, 11), (VOCAB, D), jnp.float32), -6.0, 6.0) * spread_scale
    return table


def draw_labels(key, part):
    return label_ids(key)


def draw_embedding(key, part):
    table = embed_table(key)
    table = jnp.clip(table, -2.0, 2.0)
    return table.astype(jnp.bfloat16)


def draw_hidden_states(key, part):
    row_scale = jnp.exp(jax.random.uniform(jax.random.fold_in(key, 21), (TOKENS, 1), jnp.float32, 0.0, math.log(10.0)))
    column_scale = jnp.exp(jax.random.uniform(jax.random.fold_in(key, 22), (1, D), jnp.float32, 0.0, math.log(10.0)))
    table = embed_table(key)
    spread_scale = 5.0 / math.sqrt(D)
    labels = label_ids(key)
    toward = table[labels] / spread_scale * aligned_share(key)
    values = jnp.clip(jax.random.normal(jax.random.fold_in(key, 26), (TOKENS, D), jnp.float32), -6.0, 6.0) + toward
    values = values * row_scale * column_scale
    values = jnp.clip(values, -1000.0, 1000.0)
    return values.astype(jnp.bfloat16)


def setup_inputs(seed: int = 0) -> dict:
    keys = jax.random.split(jax.random.key(seed), 5)
    hidden_states = draw_hidden_states(jax.random.fold_in(keys[4], 71), 0)
    norm_gain = jnp.clip(1.0 + 0.1 * jax.random.normal(keys[1], (D,), jnp.float32), 0.5, 1.5).astype(jnp.bfloat16)
    embedding = draw_embedding(jax.random.fold_in(keys[4], 71), 0)
    labels = draw_labels(jax.random.fold_in(keys[4], 71), 0)
    return {"hidden_states": hidden_states, "norm_gain": norm_gain, "embedding": embedding, "labels": labels}


epsilon = 1e-06

def score_rows(normed_rows, label_rows, embedding):
    logits = lax.dot_general(normed_rows, embedding, (((1,), (1,)), ((), ())), preferred_element_type=jnp.float32)
    row_max = lax.optimization_barrier(jnp.max(logits, axis=1))
    shifted = jnp.exp(logits - row_max[:, None])
    sum_exp = lax.optimization_barrier(jnp.sum(shifted, axis=1))
    sum_sq = lax.optimization_barrier(jnp.sum(shifted * shifted, axis=1))
    label_logit = jnp.take_along_axis(logits, label_rows.astype(jnp.int32)[:, None], axis=1)[:, 0]
    chance = jnp.exp(label_logit - row_max) / sum_exp
    return jnp.sqrt(sum_sq / (sum_exp * sum_exp) - 2.0 * chance + 1.0)

def reference(hidden_states, norm_gain, embedding, labels):
    widened = hidden_states.astype(jnp.float32)
    mean_sq = lax.optimization_barrier(jnp.mean(widened * widened, axis=1, keepdims=True))
    normed = (widened * lax.rsqrt(mean_sq + epsilon) * norm_gain.astype(jnp.float32)[None, :]).astype(jnp.bfloat16)
    block_rows = math.gcd(TOKENS, 512)
    blocks = TOKENS // block_rows
    normed_blocks = normed.reshape(blocks, block_rows, D)
    label_blocks = labels.reshape(blocks, block_rows)

    def one_block(pair):
        return score_rows(pair[0], pair[1], embedding)
    result = lax.map(one_block, (normed_blocks, label_blocks))
    return result.reshape(TOKENS)
```

```python
import functools
import jax
import jax.numpy as jnp
from jax import lax
from jax.experimental import pallas as pl
from jax.experimental.pallas import tpu as pltpu
from jax.sharding import PartitionSpec as P

epsilon = 1e-06
AXES = ("dp", "tensor")
CORES = 2
DIGITS = 3
EXTRA = 16
STATS = 8


def merge(parts):
    top = functools.reduce(jnp.maximum, [p[0] for p in parts])
    sum_exp, sum_sq, label = 0.0, 0.0, 0.0
    for p in parts:
        scale = jnp.exp(p[0] - top)
        sum_exp = sum_exp + p[1] * scale
        sum_sq = sum_sq + p[2] * scale * scale
        label = label + p[3]
    return top, sum_exp, sum_sq, label


def pick_chunk(rows, limit=320):
    for size in range(min(rows, limit), 0, -1):
        if rows % size == 0 and size % 8 == 0:
            return size
    return rows


def stats_kernel(slots, tables, where_ref, *refs):
    token_refs, table_refs = refs[:slots], refs[slots : slots + tables]
    out_ref, normed_ref = refs[slots + tables], refs[slots + tables + 1]
    width = token_refs[0].shape[1]
    tokens = token_refs[0].shape[0] - EXTRA
    features = width * slots
    total = jnp.zeros((tokens, 1), jnp.float32)
    for ref in token_refs:
        wide = ref[:tokens, :].astype(jnp.float32)
        total = total + jnp.sum(wide * wide, axis=1, keepdims=True)
    scale = lax.rsqrt(total / features + epsilon)
    for s, ref in enumerate(token_refs):
        wide = ref[:tokens, :].astype(jnp.float32)
        extra = ref[tokens:, :].astype(jnp.float32)
        normed = (wide * scale * extra[0:1, :]).astype(jnp.bfloat16)
        normed_ref[:, pl.ds(pl.multiple_of(where_ref[s] * width, 128), width)] = normed
    digits = token_refs[0][tokens:, :].astype(jnp.float32)
    label = digits[1:2, :] + 256.0 * digits[2:3, :] + 65536.0 * digits[3:4, :]
    label = label.astype(jnp.int32)
    normed = normed_ref[...]
    parts = []
    for i, table in enumerate(table_refs):
        rows = table.shape[0]
        chunk = pick_chunk(rows)
        ids = lax.broadcasted_iota(jnp.int32, (chunk, tokens), 0)
        for start in range(0, rows, chunk):
            logits = lax.dot_general(
                table[start : start + chunk, :],
                normed,
                (((1,), (1,)), ((), ())),
                preferred_element_type=jnp.float32,
            )
            top = jnp.max(logits, axis=0, keepdims=True)
            shifted = jnp.exp(logits - top)
            sum_exp = jnp.sum(shifted, axis=0, keepdims=True)
            sum_sq = jnp.sum(shifted * shifted, axis=0, keepdims=True)
            hit = ids == label - (where_ref[slots + i] + start)
            found = jnp.sum(jnp.where(hit, logits, 0.0), axis=0, keepdims=True)
            parts.append((top, sum_exp, sum_sq, found))
    top, sum_exp, sum_sq, found = merge(parts)
    pad = jnp.zeros((STATS - 4, tokens), jnp.float32)
    out_ref[...] = jnp.concatenate([top, sum_exp, sum_sq, found, pad], axis=0)


def block_stats(where, token_slots, tables):
    slots = len(token_slots)
    tokens = token_slots[0].shape[0] - EXTRA
    features = token_slots[0].shape[1] * slots
    rows = sum(t.shape[0] for t in tables)
    vmem = pl.BlockSpec(memory_space=pltpu.VMEM)
    return pl.pallas_call(
        functools.partial(stats_kernel, slots, len(tables)),
        out_shape=jax.ShapeDtypeStruct((STATS, tokens), jnp.float32),
        in_specs=[pl.BlockSpec(memory_space=pltpu.SMEM)] + [vmem] * (slots + len(tables)),
        out_specs=vmem,
        scratch_shapes=[pltpu.VMEM((tokens, features), jnp.bfloat16)],
        cost_estimate=pl.CostEstimate(
            flops=2 * tokens * rows * features,
            bytes_accessed=2 * (tokens + rows) * features,
            transcendentals=tokens * rows,
        ),
        name="block_stats",
    )(where, *token_slots, *tables)


def unstack(ref):
    return ref[0:1, :], ref[1:2, :], ref[2:3, :], ref[3:4, :]


def merge_kernel(final, *refs):
    out_ref = refs[-1]
    top, sum_exp, sum_sq, label = merge([unstack(r) for r in refs[:-1]])
    if final:
        chance = jnp.exp(label - top) / sum_exp
        score = jnp.sqrt(sum_sq / (sum_exp * sum_exp) - 2.0 * chance + 1.0)
        out_ref[...] = score
    else:
        pad = jnp.zeros((STATS - 4, top.shape[1]), jnp.float32)
        out_ref[...] = jnp.concatenate([top, sum_exp, sum_sq, label, pad], axis=0)


def merge_call(final, parts):
    tokens = parts[0].shape[1]
    vmem = pl.BlockSpec(memory_space=pltpu.VMEM)
    return pl.pallas_call(
        functools.partial(merge_kernel, final),
        out_shape=jax.ShapeDtypeStruct((1 if final else STATS, tokens), jnp.float32),
        in_specs=[vmem] * len(parts),
        out_specs=vmem,
        name="merge_final" if final else "merge_part",
    )(*parts)


def exchange(array, dp_count, tensor_count, dp_flip=0, tensor_flip=0):
    pairs = [
        (dp * tensor_count + t, (dp ^ dp_flip) * tensor_count + (t ^ tensor_flip))
        for dp in range(dp_count)
        for t in range(tensor_count)
    ]
    return lax.ppermute(array, AXES, pairs)


def with_extras(hidden, gain, labels):
    width = hidden.shape[1]
    digits = [(labels >> (8 * i)) & 255 for i in range(DIGITS)]
    rows = jnp.stack([gain] + [d.astype(jnp.bfloat16) for d in digits])
    pad = jnp.zeros((EXTRA - 1 - DIGITS, width), jnp.bfloat16)
    return jnp.concatenate([hidden, rows, pad], axis=0)


def planned(dp_count, tensor_count, hidden_states, norm_gain, embedding, labels):
    swap = functools.partial(exchange, dp_count=dp_count, tensor_count=tensor_count)
    x, y = CORES, 2 * CORES
    dp_index, tensor_index = lax.axis_index("dp"), lax.axis_index("tensor")
    own = with_extras(hidden_states, norm_gain, labels)
    own_slots, x_slots, y_slots, far_slots = [own], [], [], []
    x_slots.append(swap(own, dp_flip=x))
    y_slots.append(swap(own, dp_flip=y))
    own_slots.append(swap(own, tensor_flip=1))
    own_slots.append(swap(own, tensor_flip=2))
    peer_table = swap(embedding, dp_flip=1)
    x_slots.append(swap(own_slots[1], dp_flip=x))
    y_slots.append(swap(own_slots[1], dp_flip=y))
    own_slots.append(swap(own_slots[2], tensor_flip=1))
    far_slots.append(swap(y_slots[0], dp_flip=x))
    far_slots.append(swap(x_slots[1], dp_flip=y))
    for s in (2, 3):
        x_slots.append(swap(own_slots[s], dp_flip=x))
        y_slots.append(swap(own_slots[s], dp_flip=y))
    far_slots.append(swap(y_slots[2], dp_flip=x))
    far_slots.append(swap(x_slots[3], dp_flip=y))

    rows = embedding.shape[0]
    chunks = [tensor_index ^ s for s in range(tensor_count)]
    bases = [(dp * tensor_count + tensor_index) * rows for dp in (dp_index, dp_index ^ 1)]
    where = jnp.stack(chunks + bases).astype(jnp.int32)
    tables = [embedding, peer_table]
    own_stats = block_stats(where, own_slots, tables)
    x_stats = swap(block_stats(where, x_slots, tables), dp_flip=x)
    y_stats = swap(block_stats(where, y_slots, tables), dp_flip=y)
    near = merge_call(False, [own_stats, x_stats, y_stats])
    parts = [near] + [swap(near, tensor_flip=s) for s in range(1, tensor_count)]
    far = block_stats(where, far_slots, tables)
    parts += [swap(far, dp_flip=x | y, tensor_flip=s) for s in range(tensor_count)]
    return merge_call(True, parts).reshape(labels.shape)


def gathered(dp_count, tensor_count, hidden_states, norm_gain, embedding, labels):
    tokens = labels.shape[0]
    hidden = lax.all_gather(hidden_states, "tensor", axis=1, tiled=True)
    gain = lax.all_gather(norm_gain, "tensor", axis=0, tiled=True)
    table = lax.all_gather(embedding, "dp", axis=0, tiled=True)
    wide = hidden.astype(jnp.float32)
    mean_sq = jnp.mean(wide * wide, axis=1, keepdims=True)
    normed = (wide * lax.rsqrt(mean_sq + epsilon) * gain.astype(jnp.float32)[None, :]).astype(jnp.bfloat16)
    logits = lax.dot_general(normed, table, (((1,), (1,)), ((), ())), preferred_element_type=jnp.float32)
    position = jnp.arange(table.shape[0], dtype=jnp.int32)
    rows = embedding.shape[0]
    ids = (position // rows * tensor_count + lax.axis_index("tensor")) * rows + position % rows
    top = jnp.max(logits, axis=1)
    all_top = lax.pmax(top, "tensor")
    shifted = jnp.exp(logits - all_top[:, None])
    label = jnp.sum(jnp.where(ids[None, :] == labels[:, None], logits, 0.0), axis=1)
    sum_exp, sum_sq, label = lax.psum(
        (jnp.sum(shifted, axis=1), jnp.sum(shifted * shifted, axis=1), label), "tensor"
    )
    chance = jnp.exp(label - all_top) / sum_exp
    return jnp.sqrt(sum_sq / (sum_exp * sum_exp) - 2.0 * chance + 1.0)


def solution(mesh):
    dp_count, tensor_count = mesh.shape["dp"], mesh.shape["tensor"]
    fits = (dp_count, tensor_count) == (4 * CORES, 4)
    body = functools.partial(planned if fits else gathered, dp_count, tensor_count)
    in_specs = (P("dp", "tensor"), P("tensor"), P(AXES, None), P("dp"))
    return jax.shard_map(body, mesh=mesh, in_specs=in_specs, out_specs=P("dp"), check_vma=False)
```
